32 devices in a mesh: section: 2 (over x), expert: 4 (over z), tensor: 4 (over y, core).
Axes of the slice: x: 2, y: 2, z: 4, core: 2. Of those that a mesh axis runs over, the one named last changes fastest.
Arguments:
- layer_inputs: bfloat16 [2, 2, 320, 3072], P('section', None, 'expert', 'tensor'), may hold values from -6 to 6
- grad_out: bfloat16 [2, 320, 3072], P(None, 'expert', 'tensor'), may hold values from -6 to 6
- norm_gain: bfloat16 [2, 3072], P('section', 'tensor'), may hold values from 0.25 to 1.75
- router_w: bfloat16 [2, 3072, 4], P('section', 'tensor'), may hold values from -0.21875 to 0.21875
- w_gate: bfloat16 [2, 3072, 32768], P('section', None, ('expert', 'tensor')), may hold values from -0.109375 to 0.109375
- w_up: bfloat16 [2, 3072, 32768], P('section', None, ('expert', 'tensor')), may hold values from -0.109375 to 0.109375
- w_down: bfloat16 [2, 32768, 3072], P('section', ('expert', 'tensor')), may hold values from -0.0625 to 0.0625
- saved_gate: bfloat16 [2, 2, 4, 64, 32768], P('section', None, None, None, ('expert', 'tensor')), may hold values from -6 to 6
- saved_up: bfloat16 [2, 2, 4, 64, 32768], P('section', None, None, None, ('expert', 'tensor')), may hold values from -6 to 6
- routes: int32 [2, 2, 320, 2], P('section', None, 'expert'), may hold values from 0 to 3, all different within a row; in each aligned block of 80 rows (0 to 79, 80 to 159, ..., all dimensions but the last counted through in order) at most 64 rows name the same one
Outputs:
- layer_grads: bfloat16 [2, 2, 320, 3072], P('section', None, 'expert', 'tensor')
The draws below stay inside these ranges and needn't reach their ends.
Inputs may be any that keep to these rules, and one draw needn't show every extreme that they name: `routes`: each token names two different experts; within the 80 tokens of one device's aligned block of a layer and micro-batch, no expert is named by more than 64 tokens, and in some blocks one expert is named by exactly 64.
All inputs are finite; a program needn't handle non-finite values.
Results may differ from the reference program's by a relative error of at most 0.011.
Values may be sent and summed in bfloat16 or wider, within the bound.
A program may use at most 128 MiB of HBM per device.

```python
import math
import jax
import jax.numpy as jnp
import numpy as np
from jax import lax

D = 3072
FF = 8192
EXPERTS = 4
TOP = 2
MICRO = 2
TOK_DEV = 80
CAP = 64
LAYERS = 2
TOKENS = 320
N_EXPERT = 4


def levels(own_key, dims, cuts, low, largest):
    def one(dim, parts):
        steps = jax.random.uniform(jax.random.fold_in(jax.random.fold_in(own_key, 6), dim), (parts,), jnp.float32, low / len(cuts), largest / len(cuts))
        return jnp.repeat(jnp.exp(steps), dims[dim] // parts).reshape((-1,) + (1,) * (len(dims) - dim - 1))

    loudness = one(*cuts[0])
    for cut in cuts[1:]:
        loudness = loudness * one(*cut)
    return loudness


def deal_out(own_key, own, number, rows, count, top, most, lean):
    ranking = jax.random.permutation(own_key, count)
    crowded, common = portions_of(count, rows * top, most, lean, True), portions_of(count, rows * top, most, lean, False)
    places = jnp.arange(count)

    def named(sizes, turn):
        used = int((sizes > 0).sum())
        fixed = max(1, used // 4)
        shifted = fixed + (places - fixed + turn * (used - fixed)) % max(1, count - fixed)
        return jnp.zeros((count,), jnp.int32).at[ranking[jnp.where(places < fixed, places, shifted)]].set(jnp.asarray(sizes, jnp.int32))

    sizes = jnp.where(number % 4 == 0, named(crowded, number // 4), named(common, number - number // 4 - 1))
    mixed = jax.random.permutation(jax.random.fold_in(own, 3), count)
    source_of, receiver = mixed[0:count // 2 * 2:2], mixed[1:count // 2 * 2:2]
    slack = jnp.minimum(sizes[source_of] - 1, most - sizes[receiver]) // 2
    slack = jnp.where((source_of == ranking[0]) | (receiver == ranking[0]) | (sizes[receiver] == 0), 0, jnp.maximum(slack, 0))
    shifted = jax.random.randint(jax.random.fold_in(own, 4), (count // 2,), 0, 1 << 20) % (slack + 1)
    sizes = sizes.at[source_of].add(-shifted).at[receiver].add(shifted)
    labels = jnp.searchsorted(jnp.cumsum(sizes), jnp.arange(rows * top), side="right").astype(jnp.int32)
    grid = labels.reshape(top, rows).T
    grid = grid[jax.random.permutation(jax.random.fold_in(own, 1), rows)]
    turn = jax.random.randint(jax.random.fold_in(own, 2), (rows, 1), 0, top)
    return jnp.take_along_axis(grid, (jnp.arange(top)[None, :] + turn) % top, axis=1)


def portions_of(number_of, total, limit, skew, full):
    loads = [(1 << 20) // math.isqrt(rank ** skew) + 1 for rank in range(1, number_of + 1)]
    largest = limit if full else min(limit, max(-(-total // number_of), total * loads[0] // sum(loads)))
    least = 1 if total - largest >= number_of - 1 else 0
    given, surplus = [largest] + [least] * (number_of - 1), total - largest - least * (number_of - 1)
    while surplus > 0:
        free = [i for i in range(1, number_of) if given[i] < largest] or [i for i in range(1, number_of) if given[i] < limit]
        whole, left = sum([loads[i] for i in free]), surplus
        for i in free:
            addition = min(limit - given[i], max(1, left * loads[i] // whole), surplus)
            given[i] = given[i] + addition
            surplus = surplus - addition
    return np.array(given)


def scatter_about(rng, dims, spread, bound, split=(), kind=jnp.bfloat16):
    array = spread * jax.random.normal(rng, dims, jnp.float32)
    if split:
        array = array * levels(rng, dims, split, -0.22, 0.18)
    return jnp.clip(array, -bound, bound).astype(kind)


def setup_inputs(seed: int = 0) -> dict:
    key_list = jax.random.split(jax.random.key(seed), 11)
    layer_inputs = scatter_about(key_list[0], (LAYERS, MICRO, TOKENS, D), 1.0, 6.0, ((0, 2), (2, 4), (3, 4)))
    grad_out = scatter_about(key_list[1], (MICRO, TOKENS, D), 1.0, 6.0, ((1, 4), (2, 4)))
    norm_gain = jnp.clip(1.0 + 0.15 * jax.random.normal(key_list[2], (LAYERS, D), jnp.float32), 0.25, 1.75).astype(jnp.bfloat16)
    router_w = scatter_about(key_list[3], (LAYERS, D, EXPERTS), (D // 4) ** -0.5, 0.21875, ((0, 2), (1, 4)))
    w_gate = scatter_about(key_list[4], (LAYERS, D, EXPERTS * FF), D ** -0.5, 0.109375, ((0, 2), (2, 16)))
    w_up = scatter_about(key_list[5], (LAYERS, D, EXPERTS * FF), D ** -0.5, 0.109375, ((0, 2), (2, 16)))
    w_down = scatter_about(key_list[6], (LAYERS, EXPERTS * FF, D), FF ** -0.5, 0.0625, ((0, 2), (1, 16)))
    saved_gate = scatter_about(key_list[7], (LAYERS, MICRO, N_EXPERT, CAP, EXPERTS * FF), 1.0, 6.0, ((0, 2), (4, 16)))
    saved_up = scatter_about(key_list[8], (LAYERS, MICRO, N_EXPERT, CAP, EXPERTS * FF), 1.0, 6.0, ((0, 2), (4, 16)))
    routes_keys = jax.random.split(jax.random.fold_in(key_list[9], 1), LAYERS * MICRO * TOKENS // TOK_DEV)
    routes_turns = jax.random.permutation(jax.random.fold_in(key_list[9], 3), LAYERS * MICRO * TOKENS // TOK_DEV)
    routes = jax.vmap(lambda own, number: deal_out(jax.random.fold_in(key_list[9], 2), own, number, TOK_DEV, EXPERTS, TOP, CAP, 2))(routes_keys, routes_turns).reshape((LAYERS, MICRO, TOKENS, TOP))
    return {"layer_inputs": layer_inputs, "grad_out": grad_out, "norm_gain": norm_gain, "router_w": router_w, "w_gate": w_gate, "w_up": w_up, "w_down": w_down, "saved_gate": saved_gate, "saved_up": saved_up, "routes": routes}


norm_eps = 1e-05
highest = lax.Precision.HIGHEST

def layer_back(inputs, upstream, gain, router, gate_mats, up_mats, down_mats, gate_saved, up_saved, chosen):
    values = inputs.astype(jnp.float32)
    gain_full = gain.astype(jnp.float32)
    scale = lax.rsqrt(lax.optimization_barrier(jnp.mean(values * values, axis=-1, keepdims=True)) + norm_eps)
    normed = (values * scale * gain_full).astype(jnp.bfloat16)
    logits = jnp.dot(normed, router, preferred_element_type=jnp.float32)
    experts = router.shape[1]
    tokens = values.shape[0]
    senders = tokens // TOK_DEV
    onehot = (chosen[:, :, None] == jnp.arange(experts, dtype=jnp.int32)[None, None, :]).astype(jnp.float32)
    picked = lax.optimization_barrier(jnp.sum(onehot * logits[:, None, :], axis=-1))
    first = jax.nn.sigmoid(picked[:, 0] - picked[:, 1])
    second = jax.nn.sigmoid(picked[:, 1] - picked[:, 0])
    blocks = onehot.reshape(senders, TOK_DEV * 2, experts)
    earlier = jnp.cumsum(blocks, axis=1) - blocks
    within = lax.optimization_barrier(jnp.sum(earlier * blocks, axis=-1)).astype(jnp.int32).reshape(tokens, 2)
    sender = jnp.arange(tokens, dtype=jnp.int32) // TOK_DEV
    token_ids = jnp.arange(tokens, dtype=jnp.int32)
    slot_total = senders * CAP
    hidden_grad = jnp.zeros(values.shape, jnp.float32)
    prob_grad = jnp.zeros(picked.shape, jnp.float32)
    for expert in range(experts):
        mine = chosen == expert
        used = jnp.any(mine, axis=1)
        place_at = lax.optimization_barrier(jnp.sum(jnp.where(mine, within, 0), axis=1)).astype(jnp.int32)
        slot = jnp.where(used, sender * CAP + place_at, slot_total).astype(jnp.int32)
        table = jnp.zeros((slot_total + 1,), jnp.int32).at[slot].set(token_ids)[:-1]
        filled = jnp.zeros((slot_total + 1,), jnp.int32).at[slot].set(1)[:-1]
        rows = jnp.where(filled[:, None] > 0, upstream[table], jnp.zeros((), jnp.bfloat16))
        low = expert * FF
        gate_act = gate_saved[:, :, low:low + FF].reshape(slot_total, FF).astype(jnp.float32)
        up_act = up_saved[:, :, low:low + FF].reshape(slot_total, FF).astype(jnp.float32)
        back_act = jnp.dot(rows, down_mats[low:low + FF].T, preferred_element_type=jnp.float32)
        sigma = jax.nn.sigmoid(gate_act)
        swish = gate_act * sigma
        weight_grad = lax.optimization_barrier(jnp.sum(swish * up_act * back_act, axis=-1))
        slope = sigma * (1.0 + gate_act * (1.0 - sigma))
        gate_grad = (back_act * up_act * slope).astype(jnp.bfloat16)
        up_grad = (back_act * swish).astype(jnp.bfloat16)
        unit = jnp.dot(gate_grad, gate_mats[:, low:low + FF].T, preferred_element_type=jnp.float32)
        unit = unit + jnp.dot(up_grad, up_mats[:, low:low + FF].T, preferred_element_type=jnp.float32)
        reach = jnp.minimum(slot, slot_total - 1).astype(jnp.int32)
        share = first * onehot[:, 0, expert] + second * onehot[:, 1, expert]
        hidden_grad = hidden_grad + share[:, None] * unit[reach]
        prob_grad = prob_grad + onehot[:, :, expert] * weight_grad[reach][:, None]
    logit_step = first * second * (prob_grad[:, 0] - prob_grad[:, 1])
    logit_grad = (onehot[:, 0, :] - onehot[:, 1, :]) * logit_step[:, None]
    hidden_grad = hidden_grad + jnp.dot(logit_grad, router.astype(jnp.float32).T, precision=highest)
    gained = hidden_grad * gain_full
    moment = lax.optimization_barrier(jnp.mean(values * gained, axis=-1, keepdims=True))
    result = upstream.astype(jnp.float32) + scale * gained - values * scale * scale * scale * moment
    return result.astype(jnp.bfloat16)

def reference(layer_inputs, grad_out, norm_gain, router_w, w_gate, w_up, w_down, saved_gate, saved_up, routes):
    stacked = []
    for micro in range(MICRO):

        def one_layer(upstream, pieces):
            inputs, gain, router, gate_mats, up_mats, down_mats, gate_saved, up_saved, chosen = pieces
            result = layer_back(inputs, upstream, gain, router, gate_mats, up_mats, down_mats, gate_saved, up_saved, chosen)
            return (result, result)
        pieces = (layer_inputs[:, micro], norm_gain, router_w, w_gate, w_up, w_down, saved_gate[:, micro], saved_up[:, micro], routes[:, micro])
        final, series = lax.scan(one_layer, grad_out[micro], pieces, reverse=True)
        stacked.append(series)
    return jnp.stack(stacked, axis=1)
```

```python
import functools

import jax
import jax.numpy as jnp
from jax import lax
from jax.experimental import pallas as pl
from jax.experimental.pallas import tpu as pltpu
from jax.sharding import PartitionSpec as P

norm_eps = 1e-05
MESH = pl.DeviceIdType.MESH
LANES = 128
f32 = jnp.float32
bf16 = jnp.bfloat16


def vmem(count):
    return [pl.BlockSpec(memory_space=pltpu.VMEM)] * count


def remote(src, dst, send_sem, recv_sem, **where):
    return pltpu.make_async_remote_copy(
        src_ref=src,
        dst_ref=dst,
        send_sem=send_sem,
        recv_sem=recv_sem,
        device_id=where,
        device_id_type=MESH,
    )


def greet(places):
    barrier = pltpu.get_barrier_semaphore()
    for place in places:
        pl.semaphore_signal(barrier, inc=1, device_id=place, device_id_type=MESH)
    pl.semaphore_wait(barrier, len(places))


def tensor_place(T):
    t = lax.axis_index("tensor")
    core = lax.rem(t, 2)
    return t, t // 2, core


def exchange_places(H, T):
    z = lax.axis_index("expert")
    t, chip, core = tensor_place(T)
    chips = T // 2
    places = [{"expert": lax.rem(z + k, H)} for k in range(1, H)]
    places += [{"tensor": chip * 2 + 1 - core}]
    places += [{"tensor": lax.rem(chip + j, chips) * 2 + core} for j in range(1, chips)]
    return places


def dispatch_kernel(H, group, T, q, send_ref, out_ref, own_sem, zs, zr, ys, yr, cs, cr):
    z = lax.axis_index("expert")
    t, chip, core = tensor_place(T)
    chips = T // 2
    mate = chip * 2 + 1 - core

    def block(s, tt):
        return out_ref.at[s, :, pl.ds(pl.multiple_of(tt * q, LANES), q)]

    greet(exchange_places(H, T))
    own = pltpu.make_async_copy(send_ref.at[z // group], block(z, t), own_sem)
    own.start()
    far = [own]
    for k in range(1, H):
        h = lax.rem(z + k, H)
        copy = remote(send_ref.at[h // group], block(z, t), zs.at[k], zr.at[k], expert=h)
        copy.start()
        far.append(copy)
    across = {}
    beside = {}

    def relay(k):
        s = lax.rem(z - k + H, H)
        for j in range(1, chips):
            across[k, j].wait_recv()
            here = block(s, lax.rem(chip - j + chips, chips) * 2 + core)
            beside[k, j] = remote(here, here, cs.at[k, j], cr.at[k, j], tensor=mate)
            beside[k, j].start()

    for k in range(H):
        s = lax.rem(z - k + H, H)
        if k == 0:
            own.wait()
        else:
            far[k].wait_recv()
        here = block(s, t)
        for j in range(1, chips):
            to = lax.rem(chip + j, chips) * 2 + core
            across[k, j] = remote(here, here, ys.at[k, j], yr.at[k, j], tensor=to)
            across[k, j].start()
        beside[k, 0] = remote(here, here, cs.at[k, 0], cr.at[k, 0], tensor=mate)
        beside[k, 0].start()
        if k > 0:
            relay(k - 1)
    relay(H - 1)
    for copy in beside.values():
        copy.wait_recv()
    for copy in far[1:] + list(across.values()) + list(beside.values()):
        copy.wait_send()


def dispatch(send, H, T):
    experts, cap, q = send.shape
    group = H // experts
    chips = T // 2
    dma = pltpu.SemaphoreType.DMA
    return pl.pallas_call(
        functools.partial(dispatch_kernel, H, group, T, q),
        out_shape=jax.ShapeDtypeStruct((H, cap, q * T), bf16),
        in_specs=vmem(1),
        out_specs=vmem(1)[0],
        scratch_shapes=[dma, dma((H,)), dma((H,)), dma((H, chips)), dma((H, chips)), dma((H, chips)), dma((H, chips))],
        compiler_params=pltpu.CompilerParams(collective_id=0, has_side_effects=True),
        name="dispatch",
    )(send)


def experts_kernel(steps, micro_ref, rows_ref, down_ref, gate_ref, up_ref, ga_ref, ua_ref, out_ref, w_ref, acc):
    step = pl.program_id(0)
    nt = (((1,), (1,)), ((), ()))
    count = rows_ref.shape[0]
    wide = down_ref.shape[0]
    v = lax.dot_general(rows_ref[...], down_ref[...], nt, preferred_element_type=f32)
    a = ga_ref[...].reshape(count, wide).astype(f32)
    b = ua_ref[...].reshape(count, wide).astype(f32)
    sg = jax.nn.sigmoid(a)
    swish = a * sg
    vb = v * b
    part = jnp.sum(swish * vb, axis=-1, keepdims=True)
    da = (vb * (sg * (1.0 + a * (1.0 - sg)))).astype(bf16)
    db = (v * swish).astype(bf16)

    @pl.when(step == 0)
    def _():
        w_ref[...] = jnp.broadcast_to(part, w_ref.shape)

    @pl.when(step > 0)
    def _():
        w_ref[...] += jnp.broadcast_to(part, w_ref.shape)

    width = out_ref.shape[1]
    tile = 256 * max(1, width // 256 // 4) if width % 256 == 0 else width
    while width % tile:
        tile -= 256
    for low in range(0, width, tile):
        at = slice(low, low + tile)
        u = lax.dot_general(da, gate_ref[at, :], nt, preferred_element_type=f32)
        u = u + lax.dot_general(db, up_ref[at, :], nt, preferred_element_type=f32)

        @pl.when(step == 0)
        def _():
            acc[:, at] = u

        @pl.when(step > 0)
        def _():
            acc[:, at] += u

    @pl.when(step == steps - 1)
    def _():
        out_ref[...] = acc[...].astype(bf16)


def expert_backward(micro, rows, down, gate, up, saved_gate, saved_up):
    count, width = rows.shape
    units = down.shape[0]
    _, H, cap, _ = saved_gate.shape
    wide = min(256, units)
    steps = units // wide
    whole = lambda j, m: (0, 0)
    act = pl.BlockSpec((1, H, cap, wide), lambda j, m: (m[0], 0, 0, j))
    return pl.pallas_call(
        functools.partial(experts_kernel, steps),
        out_shape=(
            jax.ShapeDtypeStruct((count, width), bf16),
            jax.ShapeDtypeStruct((count, LANES), f32),
        ),
        grid_spec=pltpu.PrefetchScalarGridSpec(
            num_scalar_prefetch=1,
            grid=(steps,),
            in_specs=[
                pl.BlockSpec((count, width), whole),
                pl.BlockSpec((wide, width), lambda j, m: (j, 0)),
                pl.BlockSpec((width, wide), lambda j, m: (0, j)),
                pl.BlockSpec((width, wide), lambda j, m: (0, j)),
                act,
                act,
            ],
            out_specs=[pl.BlockSpec((count, width), whole), pl.BlockSpec((count, LANES), whole)],
            scratch_shapes=[pltpu.VMEM((count, width), f32)],
        ),
        compiler_params=pltpu.CompilerParams(vmem_limit_bytes=60 * 1024 * 1024),
        name="experts",
    )(micro, rows, down, gate, up, saved_gate, saved_up)


def combine_kernel(
    H, T, q, part_ref, w_ref, out_ref, wout_ref, rx1, tx2, rx2, tx3,
    own_sem, ws, wr, cs, cr, ys, yr, zs, zr,
):
    z = lax.axis_index("expert")
    t, chip, core = tensor_place(T)
    chips = T // 2
    mate = chip * 2 + 1 - core
    order = list(range(1, H)) + [0]

    def cols(tt):
        return pl.ds(pl.multiple_of(tt * q, LANES), q)

    greet(exchange_places(H, T))
    own = pltpu.make_async_copy(w_ref.at[z], wout_ref.at[z], own_sem)
    own.start()
    first = {}
    for k in order:
        s = lax.rem(z + k, H)
        for j in list(range(1, chips)) + [0]:
            theirs = lax.rem(chip + j, chips) * 2 + 1 - core
            first[k, j] = remote(
                part_ref.at[s, :, cols(theirs)], rx1.at[k, j], cs.at[k, j], cr.at[k, j], tensor=mate
            )
            first[k, j].start()
    weights = []
    for k in range(1, H):
        h = lax.rem(z + k, H)
        copy = remote(w_ref.at[h], wout_ref.at[z], ws.at[k], wr.at[k], expert=h)
        copy.start()
        weights.append(copy)
    second = {}
    for k in order:
        s = lax.rem(z + k, H)
        for j in range(1, chips):
            to = lax.rem(chip + j, chips) * 2 + core
            first[k, j].wait_recv()
            tx2[k, j] = (part_ref[s, :, cols(to)].astype(f32) + rx1[k, j].astype(f32)).astype(bf16)
            second[k, j] = remote(tx2.at[k, j], rx2.at[k, j], ys.at[k, j], yr.at[k, j], tensor=to)
            second[k, j].start()
    third = []
    for k in order:
        s = lax.rem(z + k, H)
        first[k, 0].wait_recv()
        total = part_ref[s, :, cols(t)].astype(f32) + rx1[k, 0].astype(f32)
        for j in range(1, chips):
            second[k, j].wait_recv()
            total = total + rx2[k, j].astype(f32)
        if k == 0:
            out_ref[z] = total.astype(bf16)
        else:
            tx3[k] = total.astype(bf16)
            copy = remote(tx3.at[k], out_ref.at[z], zs.at[k], zr.at[k], expert=s)
            copy.start()
            third.append(copy)
    own.wait()
    for copy in weights + third:
        copy.wait_recv()
    for copy in list(first.values()) + list(second.values()) + weights + third:
        copy.wait_send()


def combine(part, weights, T):
    H, cap, width = part.shape
    q = width // T
    chips = T // 2
    dma = pltpu.SemaphoreType.DMA
    many = lambda: dma((H, chips))
    return pl.pallas_call(
        functools.partial(combine_kernel, H, T, q),
        out_shape=(
            jax.ShapeDtypeStruct((H, cap, q), bf16),
            jax.ShapeDtypeStruct(weights.shape, f32),
        ),
        in_specs=vmem(2),
        out_specs=tuple(vmem(2)),
        scratch_shapes=[
            pltpu.VMEM((H, chips, cap, q), bf16),
            pltpu.VMEM((H, chips, cap, q), bf16),
            pltpu.VMEM((H, chips, cap, q), bf16),
            pltpu.VMEM((H, cap, q), bf16),
            dma, dma((H,)), dma((H,)), many(), many(), many(), many(), dma((H,)), dma((H,)),
        ],
        compiler_params=pltpu.CompilerParams(collective_id=1, has_side_effects=True),
        name="combine",
    )(part, weights)


def share(T, tx, rx, ss, rs):
    t = lax.axis_index("tensor")
    copies = []
    for k in range(1, T):
        copy = remote(tx, rx.at[k], ss.at[k], rs.at[k], tensor=lax.rem(t + k, T))
        copy.start()
        copies.append(copy)
    return copies


def tensor_sum_kernel(T, x_ref, out_ref, rx, ss, rs):
    t = lax.axis_index("tensor")
    greet([{"tensor": lax.rem(t + k, T)} for k in range(1, T)])
    copies = share(T, x_ref, rx, ss, rs)
    total = x_ref[...]
    for k, copy in enumerate(copies, 1):
        copy.wait_recv()
        total = total + rx[k]
    out_ref[...] = total
    for copy in copies:
        copy.wait_send()


def tensor_sum(x, T, number):
    rows, lanes = x.shape
    high, long = -(-rows // 8) * 8, -(-lanes // LANES) * LANES
    padded = jnp.pad(x, ((0, high - rows), (0, long - lanes)))
    dma = pltpu.SemaphoreType.DMA
    total = pl.pallas_call(
        functools.partial(tensor_sum_kernel, T),
        out_shape=jax.ShapeDtypeStruct(padded.shape, f32),
        in_specs=vmem(1),
        out_specs=vmem(1)[0],
        scratch_shapes=[pltpu.VMEM((T,) + padded.shape, f32), dma((T,)), dma((T,))],
        compiler_params=pltpu.CompilerParams(collective_id=number, has_side_effects=True),
        name="tensor_sum",
    )(padded)
    return total[:rows, :lanes]


def finish_kernel(
    T, S, width_all, hot_ref, units_ref, prob_ref, aux_ref, step_ref, x_ref, up_ref, gain_ref,
    out_ref, in_ref, tx, rx, ss, rs, send_sem, recv_sem,
):
    t = lax.axis_index("tensor")
    p = lax.axis_index("section")
    below = lax.rem(p + S - 1, S)
    above = lax.rem(p + 1, S)
    places = [{"tensor": lax.rem(t + k, T)} for k in range(1, T)]
    if S > 1:
        places.append({"section": above})
    greet(places)
    tokens = x_ref.shape[0]
    both = jnp.dot(hot_ref[...], units_ref[...], preferred_element_type=f32)
    aux = aux_ref[...]
    q0, q1 = aux[:, 0:1], aux[:, 1:2]
    scale, cross = aux[:, 2:3], aux[:, 3:4]
    values = x_ref[...].astype(f32)
    gain = gain_ref[...]
    hidden = q0 * both[:tokens] + q1 * both[tokens:]
    gained = hidden * gain
    moment = jnp.sum(values * gained, axis=-1, keepdims=True)
    lane = lax.broadcasted_iota(jnp.int32, prob_ref.shape, 1)
    tx[...] = jnp.where(lane == 1, moment, prob_ref[...])
    copies = share(T, tx, rx, ss, rs)
    total = tx[...]
    for k, copy in enumerate(copies, 1):
        copy.wait_recv()
        total = total + rx[k]
    step = q0 * q1 * total[:, 0:1]
    mean = (total[:, 1:2] + step * cross) / width_all
    result = (
        up_ref[...].astype(f32)
        + scale * (gained + (step * step_ref[...]) * gain)
        - values * (scale * scale * scale * mean)
    )
    out_ref[...] = result.astype(bf16)
    if S > 1:
        onward = remote(out_ref, in_ref, send_sem, recv_sem, section=below)
        onward.start()
        onward.wait()
    else:
        in_ref[...] = out_ref[...]
    for copy in copies:
        copy.wait_send()


def finish(T, S, hot, units, prob, aux, step, x, up, gain):
    tokens, q = x.shape
    shape = jax.ShapeDtypeStruct((tokens, q), bf16)
    dma = pltpu.SemaphoreType.DMA
    return pl.pallas_call(
        functools.partial(finish_kernel, T, S, q * T),
        out_shape=(shape, shape),
        in_specs=vmem(8),
        out_specs=tuple(vmem(2)),
        scratch_shapes=[
            pltpu.VMEM((tokens, LANES), f32),
            pltpu.VMEM((T, tokens, LANES), f32),
            dma((T,)), dma((T,)), dma, dma,
        ],
        compiler_params=pltpu.CompilerParams(collective_id=2, has_side_effects=True),
        name="finish",
    )(hot, units, prob, aux, step, x, up, gain)


def on_device(
    layer_inputs, grad_out, norm_gain, router_w, w_gate, w_up, w_down, saved_gate, saved_up, routes
):
    S = lax.axis_size("section")
    H = lax.axis_size("expert")
    T = lax.axis_size("tensor")
    position = lax.axis_index("section")
    micros, tokens, q = grad_out.shape
    gain = norm_gain[0].astype(f32)
    router = router_w[0]
    width = w_gate.shape[1]
    experts = router.shape[1]
    group = H // experts
    cap = saved_gate.shape[3]
    slots = experts * cap
    highest = lax.Precision.HIGHEST

    values = layer_inputs[0].astype(f32)
    router32 = router.astype(f32)
    gained_router = gain[:, None] * router32
    squares = jnp.sum(values * values, axis=-1).reshape(1, micros * tokens)
    crossing = jnp.einsum("mtd,de->emt", values, gained_router, precision=highest)
    stats = jnp.concatenate([squares, crossing.reshape(experts, micros * tokens)], axis=0)
    stats = tensor_sum(stats, T, 3)
    scale = lax.rsqrt(stats[0].reshape(micros, tokens) / width + norm_eps)
    crossing = stats[1:].reshape(experts, micros, tokens).transpose(1, 2, 0)
    normed = (values * scale[:, :, None] * gain).astype(bf16)
    logits = jnp.einsum("mtd,de->emt", normed, router, preferred_element_type=f32)
    logits = tensor_sum(logits.reshape(experts, micros * tokens), T, 4)
    logits = logits.reshape(experts, micros, tokens).transpose(1, 2, 0)

    chosen = routes[0]
    expert_ids = jnp.arange(experts, dtype=jnp.int32)
    onehot = (chosen[..., None] == expert_ids).astype(f32)
    picked = jnp.sum(onehot * logits[:, :, None, :], axis=-1)
    first = jax.nn.sigmoid(picked[..., 0] - picked[..., 1])
    second = jax.nn.sigmoid(picked[..., 1] - picked[..., 0])
    lean = onehot[:, :, 0] - onehot[:, :, 1]
    cross = jnp.sum(lean * crossing, axis=-1)
    steps = jnp.einsum("mte,de->mtd", lean, router32, precision=highest)
    flat = onehot.reshape(micros, tokens * 2, experts)
    earlier = jnp.cumsum(flat, axis=1) - flat
    within = jnp.sum(earlier * flat, axis=-1).astype(jnp.int32).reshape(micros, tokens, 2)
    target = (chosen * cap + within).transpose(0, 2, 1)
    slot_ids = jnp.arange(slots, dtype=jnp.int32)
    hot = target[..., None] == slot_ids
    select = jnp.any(hot, axis=1).astype(bf16)
    hot = hot.astype(bf16)
    wide_hot = jnp.broadcast_to(
        hot.reshape(micros, 2, tokens, experts, 1, cap), (micros, 2, tokens, experts, group, cap)
    ).reshape(micros, 2 * tokens, H * cap)
    hot_lean = (hot[:, 0].astype(f32) - hot[:, 1].astype(f32))
    aux = jnp.stack([first, second, scale, cross], axis=-1)
    aux = jnp.pad(aux, ((0, 0), (0, 0), (0, LANES - 4)))

    def pick(array, number):
        return lax.dynamic_index_in_dim(array, number, 0, keepdims=False)

    lanes = -(-cap // LANES) * LANES
    incoming = jnp.zeros((tokens, q), bf16)
    grads = jnp.zeros((micros, tokens, q), bf16)
    for tick in range(micros + S - 1):
        number = tick - (S - 1 - position)
        valid = jnp.logical_and(number >= 0, number < micros)
        safe = jnp.clip(number, 0, micros - 1)
        upstream = jnp.where(position == S - 1, pick(grad_out, safe), incoming)
        send = lax.dot_general(
            pick(select, safe), upstream, (((0,), (0,)), ((), ())), preferred_element_type=f32
        ).astype(bf16)
        rows = dispatch(send.reshape(experts, cap, q), H, T).reshape(H * cap, width)
        part, weight = expert_backward(
            safe[None].astype(jnp.int32), rows, w_down[0], w_gate[0], w_up[0], saved_gate[0], saved_up[0]
        )
        weight = weight[:, 0].reshape(H, 1, cap)
        weight = jnp.pad(weight, ((0, 0), (0, 7), (0, lanes - cap)))
        units, weight = combine(part.reshape(H, cap, width), weight, T)
        weight = jnp.sum(weight[:, 0, :cap].reshape(experts, group, cap), axis=1).reshape(slots)
        prob = jnp.sum(pick(hot_lean, safe) * weight[None, :], axis=-1, keepdims=True)
        prob = jnp.pad(prob, ((0, 0), (0, LANES - 1)))
        result, incoming = finish(
            T, S, pick(wide_hot, safe), units.reshape(H * cap, q), prob, pick(aux, safe),
            pick(steps, safe), pick(layer_inputs[0], safe), upstream, gain[None, :],
        )
        updated = lax.dynamic_update_index_in_dim(grads, result, safe, 0)
        grads = jnp.where(valid, updated, grads)
    return grads[None]


def solution(mesh):
    placed = (
        P("section", None, "expert", "tensor"),
        P(None, "expert", "tensor"),
        P("section", "tensor"),
        P("section", "tensor", None),
        P("section", None, ("expert", "tensor")),
        P("section", None, ("expert", "tensor")),
        P("section", ("expert", "tensor"), None),
        P("section", None, None, None, ("expert", "tensor")),
        P("section", None, None, None, ("expert", "tensor")),
        P("section", None, "expert", None),
    )
    return jax.shard_map(
        on_device,
        mesh=mesh,
        in_specs=placed,
        out_specs=P("section", None, "expert", "tensor"),
        check_vma=False,
    )
```

```python
import functools

import jax
import jax.numpy as jnp
from jax import lax
from jax.experimental import pallas as pl
from jax.experimental.pallas import tpu as pltpu
from jax.sharding import PartitionSpec as P

norm_eps = 1e-05
MESH = pl.DeviceIdType.MESH
LANES = 128
f32 = jnp.float32
bf16 = jnp.bfloat16


def vmem(count):
    return [pl.BlockSpec(memory_space=pltpu.VMEM)] * count


def remote(src, dst, send_sem, recv_sem, **where):
    return pltpu.make_async_remote_copy(
        src_ref=src,
        dst_ref=dst,
        send_sem=send_sem,
        recv_sem=recv_sem,
        device_id=where,
        device_id_type=MESH,
    )


def greet(places):
    barrier = pltpu.get_barrier_semaphore()
    for place in places:
        pl.semaphore_signal(barrier, inc=1, device_id=place, device_id_type=MESH)
    pl.semaphore_wait(barrier, len(places))


def tensor_place(T):
    t = lax.axis_index("tensor")
    core = lax.rem(t, 2)
    return t, t // 2, core


def exchange_places(H, T):
    z = lax.axis_index("expert")
    t, chip, core = tensor_place(T)
    chips = T // 2
    places = [{"expert": lax.rem(z + k, H)} for k in range(1, H)]
    places += [{"tensor": chip * 2 + 1 - core}]
    places += [{"tensor": lax.rem(chip + j, chips) * 2 + core} for j in range(1, chips)]
    return places


def dispatch_kernel(H, group, T, q, send_ref, out_ref, own_sem, zs, zr, ys, yr, cs, cr):
    z = lax.axis_index("expert")
    t, chip, core = tensor_place(T)
    chips = T // 2
    mate = chip * 2 + 1 - core

    def block(s, tt):
        return out_ref.at[s, :, pl.ds(pl.multiple_of(tt * q, LANES), q)]

    greet(exchange_places(H, T))
    own = pltpu.make_async_copy(send_ref.at[z // group], block(z, t), own_sem)
    own.start()
    far = [own]
    for k in range(1, H):
        h = lax.rem(z + k, H)
        copy = remote(send_ref.at[h // group], block(z, t), zs.at[k], zr.at[k], expert=h)
        copy.start()
        far.append(copy)
    across = {}
    beside = {}

    def relay(k):
        s = lax.rem(z - k + H, H)
        for j in range(1, chips):
            across[k, j].wait_recv()
            here = block(s, lax.rem(chip - j + chips, chips) * 2 + core)
            beside[k, j] = remote(here, here, cs.at[k, j], cr.at[k, j], tensor=mate)
            beside[k, j].start()

    for k in range(H):
        s = lax.rem(z - k + H, H)
        if k == 0:
            own.wait()
        else:
            far[k].wait_recv()
        here = block(s, t)
        for j in range(1, chips):
            to = lax.rem(chip + j, chips) * 2 + core
            across[k, j] = remote(here, here, ys.at[k, j], yr.at[k, j], tensor=to)
            across[k, j].start()
        beside[k, 0] = remote(here, here, cs.at[k, 0], cr.at[k, 0], tensor=mate)
        beside[k, 0].start()
        if k > 0:
            relay(k - 1)
    relay(H - 1)
    for copy in beside.values():
        copy.wait_recv()
    for copy in far[1:] + list(across.values()) + list(beside.values()):
        copy.wait_send()


def dispatch(send, H, T):
    experts, cap, q = send.shape
    group = H // experts
    chips = T // 2
    dma = pltpu.SemaphoreType.DMA
    return pl.pallas_call(
        functools.partial(dispatch_kernel, H, group, T, q),
        out_shape=jax.ShapeDtypeStruct((H, cap, q * T), bf16),
        in_specs=vmem(1),
        out_specs=vmem(1)[0],
        scratch_shapes=[dma, dma((H,)), dma((H,)), dma((H, chips)), dma((H, chips)), dma((H, chips)), dma((H, chips))],
        compiler_params=pltpu.CompilerParams(collective_id=0, has_side_effects=True),
        name="dispatch",
    )(send)


def experts_kernel(steps, micro_ref, rows_ref, down_ref, gate_ref, up_ref, ga_ref, ua_ref, out_ref, w_ref, acc):
    step = pl.program_id(0)
    nt = (((1,), (1,)), ((), ()))
    count, width = rows_ref.shape
    wide = down_ref.shape[0]
    v = lax.dot_general(rows_ref[...], down_ref[...], nt, preferred_element_type=f32)
    a = ga_ref[...].reshape(count, wide).astype(f32)
    b = ua_ref[...].reshape(count, wide).astype(f32)
    sg = jax.nn.sigmoid(a)
    swish = a * sg
    vb = v * b
    part = jnp.sum(swish * vb, axis=-1, keepdims=True)
    da = (vb * (sg * (1.0 + a * (1.0 - sg)))).astype(bf16)
    db = (v * swish).astype(bf16)
    dab = jnp.concatenate([da, db], axis=1)

    @pl.when(step == 0)
    def _():
        w_ref[...] = jnp.broadcast_to(part, w_ref.shape)
        acc[...] = jnp.zeros_like(acc)

    @pl.when(step > 0)
    def _():
        w_ref[...] += jnp.broadcast_to(part, w_ref.shape)

    tile = next(n for n in (256, 768, 512, 384, 256, 128, width) if width % n == 0)
    for low in range(0, width, tile):
        at = slice(low, low + tile)
        acc[:, at] += lax.dot_general(dab, jnp.concatenate([gate_ref[at, :], up_ref[at, :]], axis=1), nt, preferred_element_type=f32)

    @pl.when(step == steps - 1)
    def _():
        for low in range(0, width, LANES):
            at = slice(low, low + LANES)
            out_ref[:, at] = acc[:, at].astype(bf16)


def expert_backward(micro, rows, down, gate, up, saved_gate, saved_up):
    count, width = rows.shape
    units = down.shape[0]
    _, H, cap, _ = saved_gate.shape
    wide = min(512 if count <= 512 else 256, units)
    steps = units // wide
    whole = lambda j, m: (0, 0)
    act = pl.BlockSpec((1, H, cap, wide), lambda j, m: (m[0], 0, 0, j))
    return pl.pallas_call(
        functools.partial(experts_kernel, steps),
        out_shape=(
            jax.ShapeDtypeStruct((count, width), bf16),
            jax.ShapeDtypeStruct((count, LANES), f32),
        ),
        grid_spec=pltpu.PrefetchScalarGridSpec(
            num_scalar_prefetch=1,
            grid=(steps,),
            in_specs=[
                pl.BlockSpec((count, width), whole),
                pl.BlockSpec((wide, width), lambda j, m: (j, 0)),
                pl.BlockSpec((width, wide), lambda j, m: (0, j)),
                pl.BlockSpec((width, wide), lambda j, m: (0, j)),
                act,
                act,
            ],
            out_specs=[pl.BlockSpec((count, width), whole), pl.BlockSpec((count, LANES), whole)],
            scratch_shapes=[pltpu.VMEM((count, width), f32)],
        ),
        compiler_params=pltpu.CompilerParams(vmem_limit_bytes=60 * 1024 * 1024),
        name="experts",
    )(micro, rows, down, gate, up, saved_gate, saved_up)


def combine_kernel(
    H, T, q, part_ref, w_ref, out_ref, wout_ref, rx1, tx2, rx2, tx3,
    own_sem, ws, wr, cs, cr, ys, yr, zs, zr,
):
    z = lax.axis_index("expert")
    t, chip, core = tensor_place(T)
    chips = T // 2
    mate = chip * 2 + 1 - core
    order = list(range(1, H)) + [0]

    def cols(tt):
        return pl.ds(pl.multiple_of(tt * q, LANES), q)

    greet(exchange_places(H, T))
    own = pltpu.make_async_copy(w_ref.at[z], wout_ref.at[z], own_sem)
    own.start()
    first = {}
    for k in order:
        s = lax.rem(z + k, H)
        for j in list(range(1, chips)) + [0]:
            theirs = lax.rem(chip + j, chips) * 2 + 1 - core
            first[k, j] = remote(
                part_ref.at[s, :, cols(theirs)], rx1.at[k, j], cs.at[k, j], cr.at[k, j], tensor=mate
            )
            first[k, j].start()
    weights = []
    for k in range(1, H):
        h = lax.rem(z + k, H)
        copy = remote(w_ref.at[h], wout_ref.at[z], ws.at[k], wr.at[k], expert=h)
        copy.start()
        weights.append(copy)
    second = {}
    for k in order:
        s = lax.rem(z + k, H)
        for j in range(1, chips):
            to = lax.rem(chip + j, chips) * 2 + core
            first[k, j].wait_recv()
            tx2[k, j] = (part_ref[s, :, cols(to)].astype(f32) + rx1[k, j].astype(f32)).astype(bf16)
            second[k, j] = remote(tx2.at[k, j], rx2.at[k, j], ys.at[k, j], yr.at[k, j], tensor=to)
            second[k, j].start()
    third = []
    for k in order:
        s = lax.rem(z + k, H)
        first[k, 0].wait_recv()
        total = part_ref[s, :, cols(t)].astype(f32) + rx1[k, 0].astype(f32)
        for j in range(1, chips):
            second[k, j].wait_recv()
            total = total + rx2[k, j].astype(f32)
        if k == 0:
            out_ref[z] = total.astype(bf16)
        else:
            tx3[k] = total.astype(bf16)
            copy = remote(tx3.at[k], out_ref.at[z], zs.at[k], zr.at[k], expert=s)
            copy.start()
            third.append(copy)
    own.wait()
    for copy in weights + third:
        copy.wait_recv()
    for copy in list(first.values()) + list(second.values()) + weights + third:
        copy.wait_send()


def combine(part, weights, T):
    H, cap, width = part.shape
    q = width // T
    chips = T // 2
    dma = pltpu.SemaphoreType.DMA
    many = lambda: dma((H, chips))
    return pl.pallas_call(
        functools.partial(combine_kernel, H, T, q),
        out_shape=(
            jax.ShapeDtypeStruct((H, cap, q), bf16),
            jax.ShapeDtypeStruct(weights.shape, f32),
        ),
        in_specs=vmem(2),
        out_specs=tuple(vmem(2)),
        scratch_shapes=[
            pltpu.VMEM((H, chips, cap, q), bf16),
            pltpu.VMEM((H, chips, cap, q), bf16),
            pltpu.VMEM((H, chips, cap, q), bf16),
            pltpu.VMEM((H, cap, q), bf16),
            dma, dma((H,)), dma((H,)), many(), many(), many(), many(), dma((H,)), dma((H,)),
        ],
        compiler_params=pltpu.CompilerParams(collective_id=1, has_side_effects=True),
        name="combine",
    )(part, weights)


def share(T, tx, rx, ss, rs):
    t = lax.axis_index("tensor")
    copies = []
    for k in range(1, T):
        copy = remote(tx, rx.at[k], ss.at[k], rs.at[k], tensor=lax.rem(t + k, T))
        copy.start()
        copies.append(copy)
    return copies


def tensor_sum_kernel(T, x_ref, out_ref, rx, ss, rs):
    t = lax.axis_index("tensor")
    greet([{"tensor": lax.rem(t + k, T)} for k in range(1, T)])
    copies = share(T, x_ref, rx, ss, rs)
    total = x_ref[...]
    for k, copy in enumerate(copies, 1):
        copy.wait_recv()
        total = total + rx[k]
    out_ref[...] = total
    for copy in copies:
        copy.wait_send()


def tensor_sum(x, T, number):
    rows, lanes = x.shape
    high, long = -(-rows // 8) * 8, -(-lanes // LANES) * LANES
    padded = jnp.pad(x, ((0, high - rows), (0, long - lanes)))
    dma = pltpu.SemaphoreType.DMA
    total = pl.pallas_call(
        functools.partial(tensor_sum_kernel, T),
        out_shape=jax.ShapeDtypeStruct(padded.shape, f32),
        in_specs=vmem(1),
        out_specs=vmem(1)[0],
        scratch_shapes=[pltpu.VMEM((T,) + padded.shape, f32), dma((T,)), dma((T,))],
        compiler_params=pltpu.CompilerParams(collective_id=number, has_side_effects=True),
        name="tensor_sum",
    )(padded)
    return total[:rows, :lanes]


def finish_kernel(
    T, S, width_all, onward_too, hot_ref, units_ref, prob_ref, aux_ref, step_ref, x_ref, up_ref, gain_ref,
    out_ref, in_ref, tx, rx, ss, rs, send_sem, recv_sem,
):
    t = lax.axis_index("tensor")
    p = lax.axis_index("section")
    below = lax.rem(p + S - 1, S)
    above = lax.rem(p + 1, S)
    places = [{"tensor": lax.rem(t + k, T)} for k in range(1, T)]
    if onward_too:
        places.append({"section": above})
    greet(places)
    tokens = x_ref.shape[0]
    both = jnp.dot(hot_ref[...], units_ref[...], preferred_element_type=f32)
    aux = aux_ref[...]
    q0, q1 = aux[:, 0:1], aux[:, 1:2]
    scale, cross = aux[:, 2:3], aux[:, 3:4]
    values = x_ref[...].astype(f32)
    gain = gain_ref[...]
    hidden = q0 * both[:tokens] + q1 * both[tokens:]
    gained = hidden * gain
    moment = jnp.sum(values * gained, axis=-1, keepdims=True)
    lane = lax.broadcasted_iota(jnp.int32, prob_ref.shape, 1)
    tx[...] = jnp.where(lane == 1, moment, prob_ref[...])
    copies = share(T, tx, rx, ss, rs)
    total = tx[...]
    for k, copy in enumerate(copies, 1):
        copy.wait_recv()
        total = total + rx[k]
    step = q0 * q1 * total[:, 0:1]
    mean = (total[:, 1:2] + step * cross) / width_all
    result = (
        up_ref[...].astype(f32)
        + scale * (gained + (step * step_ref[...]) * gain)
        - values * (scale * scale * scale * mean)
    )
    out_ref[...] = result.astype(bf16)
    if onward_too:
        onward = remote(out_ref, in_ref, send_sem, recv_sem, section=below)
        onward.start()
        onward.wait()
    else:
        in_ref[...] = jnp.zeros_like(in_ref)
    for copy in copies:
        copy.wait_send()


def finish(T, S, onward_too, hot, units, prob, aux, step, x, up, gain):
    tokens, q = x.shape
    shape = jax.ShapeDtypeStruct((tokens, q), bf16)
    dma = pltpu.SemaphoreType.DMA
    return pl.pallas_call(
        functools.partial(finish_kernel, T, S, q * T, onward_too),
        out_shape=(shape, shape),
        in_specs=vmem(8),
        out_specs=tuple(vmem(2)),
        scratch_shapes=[
            pltpu.VMEM((tokens, LANES), f32),
            pltpu.VMEM((T, tokens, LANES), f32),
            dma((T,)), dma((T,)), dma, dma,
        ],
        compiler_params=pltpu.CompilerParams(collective_id=2 if onward_too else 5, has_side_effects=True),
        name="finish",
    )(hot, units, prob, aux, step, x, up, gain)


def on_device(
    layer_inputs, grad_out, norm_gain, router_w, w_gate, w_up, w_down, saved_gate, saved_up, routes
):
    S = lax.axis_size("section")
    H = lax.axis_size("expert")
    T = lax.axis_size("tensor")
    position = lax.axis_index("section")
    micros, tokens, q = grad_out.shape
    gain = norm_gain[0].astype(f32)
    router = router_w[0]
    width = w_gate.shape[1]
    experts = router.shape[1]
    group = H // experts
    cap = saved_gate.shape[3]
    slots = experts * cap
    highest = lax.Precision.HIGHEST

    values = layer_inputs[0].astype(f32)
    router32 = router.astype(f32)
    gained_router = gain[:, None] * router32
    squares = jnp.sum(values * values, axis=-1).reshape(1, micros * tokens)
    crossing = jnp.einsum("mtd,de->emt", values, gained_router, precision=highest)
    stats = jnp.concatenate([squares, crossing.reshape(experts, micros * tokens)], axis=0)
    stats = tensor_sum(stats, T, 3)
    scale = lax.rsqrt(stats[0].reshape(micros, tokens) / width + norm_eps)
    crossing = stats[1:].reshape(experts, micros, tokens).transpose(1, 2, 0)
    normed = (values * scale[:, :, None] * gain).astype(bf16)
    logits = jnp.einsum("mtd,de->emt", normed, router, preferred_element_type=f32)
    logits = tensor_sum(logits.reshape(experts, micros * tokens), T, 4)
    logits = logits.reshape(experts, micros, tokens).transpose(1, 2, 0)

    chosen = routes[0]
    expert_ids = jnp.arange(experts, dtype=jnp.int32)
    onehot = (chosen[..., None] == expert_ids).astype(f32)
    picked = jnp.sum(onehot * logits[:, :, None, :], axis=-1)
    first = jax.nn.sigmoid(picked[..., 0] - picked[..., 1])
    second = jax.nn.sigmoid(picked[..., 1] - picked[..., 0])
    lean = onehot[:, :, 0] - onehot[:, :, 1]
    cross = jnp.sum(lean * crossing, axis=-1)
    steps = jnp.einsum("mte,de->mtd", lean, router32, precision=highest)
    flat = onehot.reshape(micros, tokens * 2, experts)
    earlier = jnp.cumsum(flat, axis=1) - flat
    within = jnp.sum(earlier * flat, axis=-1).astype(jnp.int32).reshape(micros, tokens, 2)
    target = (chosen * cap + within).transpose(0, 2, 1)
    slot_ids = jnp.arange(slots, dtype=jnp.int32)
    hot = target[..., None] == slot_ids
    select = jnp.any(hot, axis=1).astype(bf16)
    hot = hot.astype(bf16)
    wide_hot = jnp.broadcast_to(
        hot.reshape(micros, 2, tokens, experts, 1, cap), (micros, 2, tokens, experts, group, cap)
    ).reshape(micros, 2 * tokens, H * cap)
    hot_lean = (hot[:, 0].astype(f32) - hot[:, 1].astype(f32))
    aux = jnp.stack([first, second, scale, cross], axis=-1)
    aux = jnp.pad(aux, ((0, 0), (0, 0), (0, LANES - 4)))

    def pick(array, number):
        return lax.dynamic_index_in_dim(array, number, 0, keepdims=False)

    lanes = -(-cap // LANES) * LANES
    incoming = jnp.zeros((tokens, q), bf16)
    grads = jnp.zeros((micros, tokens, q), bf16)
    for tick in range(micros + S - 1):
        number = tick - (S - 1 - position)
        valid = jnp.logical_and(number >= 0, number < micros)
        safe = jnp.clip(number, 0, micros - 1)
        upstream = jnp.where(position == S - 1, pick(grad_out, safe), incoming)
        send = lax.dot_general(
            pick(select, safe), upstream, (((0,), (0,)), ((), ())), preferred_element_type=f32
        ).astype(bf16)
        rows = dispatch(send.reshape(experts, cap, q), H, T).reshape(H * cap, width)
        part, weight = expert_backward(
            safe[None].astype(jnp.int32), rows, w_down[0], w_gate[0], w_up[0], saved_gate[0], saved_up[0]
        )
        weight = weight[:, 0].reshape(H, 1, cap)
        weight = jnp.pad(weight, ((0, 0), (0, 7), (0, lanes - cap)))
        units, weight = combine(part.reshape(H, cap, width), weight, T)
        weight = jnp.sum(weight[:, 0, :cap].reshape(experts, group, cap), axis=1).reshape(slots)
        prob = jnp.sum(pick(hot_lean, safe) * weight[None, :], axis=-1, keepdims=True)
        prob = jnp.pad(prob, ((0, 0), (0, LANES - 1)))
        result, incoming = finish(
            T, S, S > 1 and tick < micros + S - 2, pick(wide_hot, safe), units.reshape(H * cap, q), prob, pick(aux, safe),
            pick(steps, safe), pick(layer_inputs[0], safe), upstream, gain[None, :],
        )
        updated = lax.dynamic_update_index_in_dim(grads, result, safe, 0)
        grads = jnp.where(valid, updated, grads)
    return grads[None]


def solution(mesh):
    placed = (
        P("section", None, "expert", "tensor"),
        P(None, "expert", "tensor"),
        P("section", "tensor"),
        P("section", "tensor", None),
        P("section", None, ("expert", "tensor")),
        P("section", None, ("expert", "tensor")),
        P("section", ("expert", "tensor"), None),
        P("section", None, None, None, ("expert", "tensor")),
        P("section", None, None, None, ("expert", "tensor")),
        P("section", None, "expert", None),
    )
    return jax.shard_map(
        on_device,
        mesh=mesh,
        in_specs=placed,
        out_specs=P("section", None, "expert", "tensor"),
        check_vma=False,
    )
```
